32 devices in a mesh: depth: 2 (over core), lat: 16 (over z, y, x).
Axes of the slice: x: 2, y: 2, z: 4, core: 2. Of those that a mesh axis runs over, the one named last changes fastest.
Arguments:
- temp_old: float32 [256, 64, 512], P('depth', 'lat'), may hold values from -6 to 6
- source: float32 [256, 64, 512], P('depth', 'lat'), may hold values from -6 to 6
- lat_couple: float32 [256], P('depth'), may hold values from 0.05 to 0.2
- face_couple: float32 [1], replicated, may hold values from 0.5 to 2
- block_inverse: float32 [256, 128], P('depth'), may hold values from -0.3 to 1.4
Outputs:
- temp_new: float32 [256, 64, 512], P('depth', 'lat')
The draws below stay inside these ranges and needn't reach their ends.
All inputs are finite; a program needn't handle non-finite values.
Results may differ from the reference program's by a relative error of at most 0.0001.
Values sent between devices are 32-bit elements; how exact they have to be, the bound alone decides.
A program may use at most 64 MiB of HBM per device.

```python
import math
import jax
import jax.numpy as jnp
from jax import lax

CZ = 128
NY = 512
SWEEPS = 6
NZ = 256
NX = 64
N_DEPTH = 2


def draw_block_inverse(key, part):
    subkeys = jax.random.split(jax.random.fold_in(key, 17), 3)
    row_layer = jnp.arange(NZ) % CZ
    columns = jnp.arange(CZ)
    on_diagonal = (row_layer[:, None] == columns[None, :]).astype(jnp.float32)
    at_first = (columns[None, :] == 0).astype(jnp.float32)
    diagonal_gain = jnp.exp(jax.random.uniform(subkeys[0], (NZ,), jnp.float32, math.log(0.3), math.log(0.6)))
    spread_noise = jnp.clip(jax.random.normal(subkeys[1], (NZ, CZ), jnp.float32), -1.7, 1.7)
    first_weight = jax.random.uniform(subkeys[2], (NZ,), jnp.float32, 0.25, 0.45)
    matrix = on_diagonal * diagonal_gain[:, None] + spread_noise * (0.1 / math.sqrt(CZ)) + at_first * first_weight[:, None]
    return matrix.astype(jnp.float32)


def block_scale(key, shape, shards, low, top_value):
    level = 1.0
    for axis_at, parts in shards:
        steps = jax.random.uniform(jax.random.fold_in(jax.random.fold_in(key, 6), axis_at), (parts,), jnp.float32, low / len(shards), top_value / len(shards))
        level = level * jnp.repeat(jnp.exp(steps), shape[axis_at] // parts).reshape((-1,) + (1,) * (len(shape) - 1 - axis_at))
    return level


def centred(key, dims, scale, limit, cuts=(), held_as=jnp.bfloat16):
    array = jax.random.normal(key, dims, jnp.float32) * scale
    if len(cuts) > 0:
        array = block_scale(key, dims, cuts, -0.22, 0.18) * array
    return jnp.clip(array, min=-limit, max=limit).astype(held_as)


def setup_inputs(seed: int = 0) -> dict:
    keys = jax.random.split(jax.random.key(seed), 6)
    return {
        "temp_old": centred(keys[0], (NZ, NX, NY), 1.0, 6.0, ((0, 2), (1, 16)), jnp.float32),
        "source": centred(keys[1], (NZ, NX, NY), 1.0, 6.0, ((0, 2), (1, 16)), jnp.float32),
        "lat_couple": jnp.clip(jnp.exp(math.log(0.2) - 1.3862944 * jax.random.uniform(keys[2], (NZ,), jnp.float32) ** block_scale(keys[2], (NZ,), ((0, 2),), -0.2, 0.2)), 0.05, 0.2),
        "face_couple": jnp.clip(jnp.exp(jax.random.uniform(keys[3], (N_DEPTH - 1,), jnp.float32, math.log(0.5), math.log(2.0))), 0.5, 2.0),
        "block_inverse": draw_block_inverse(jax.random.fold_in(keys[5], 71), 0),
    }


def lateral_sum(field):
    padded = jnp.pad(field, ((0, 0), (1, 1), (1, 1)))
    return padded[:, 2:, 1:-1] + padded[:, :-2, 1:-1] + padded[:, 1:-1, 2:] + padded[:, 1:-1, :-2]


def reference(temp_old, source, lat_couple, face_couple, block_inverse):
    field = temp_old
    for sweep_index in range(SWEEPS):
        right_side = source + lat_couple[:, None, None] * lateral_sum(field)
        pieces = []
        carry = jnp.zeros(field.shape[1:], jnp.float32)
        for slab_index in range(N_DEPTH):
            slab_rhs = right_side[slab_index * CZ:(slab_index + 1) * CZ]
            if slab_index + 1 < N_DEPTH:
                slab_rhs = slab_rhs.at[CZ - 1].add(face_couple[slab_index] * field[(slab_index + 1) * CZ])
            if slab_index > 0:
                slab_rhs = slab_rhs.at[0].add(face_couple[slab_index - 1] * carry)
            inverse = block_inverse[slab_index * CZ:(slab_index + 1) * CZ]
            solved = jnp.dot(inverse, slab_rhs.reshape(CZ, -1), precision=lax.Precision.HIGHEST,
                             preferred_element_type=jnp.float32).reshape(slab_rhs.shape)
            carry = solved[CZ - 1]
            pieces.append(solved)
        field = jnp.concatenate(pieces, 0)
    return field
```

```python
import functools

import jax
import jax.numpy as jnp
from jax import lax
from jax.experimental import pallas as pl
from jax.experimental.pallas import tpu as pltpu
from jax.sharding import PartitionSpec as P

SWEEPS = 6
LANES = 128
MESH = pl.DeviceIdType.MESH
F32, BF16 = jnp.float32, jnp.bfloat16


def halves(value):
    high = value.astype(BF16)
    return high, (value - high.astype(F32)).astype(BF16)


def kernel(lat_count, temp, source, couple, face, inverse, out, field, src, above_below, sides, layer,
           side_out, layer_out, weights, matrix, local_sem, in_send, in_recv, row_send, row_recv,
           side_send, side_recv, layer_send, layer_recv, out_send, out_recv):
    tile_rows, depth, cols = temp.shape
    group = cols // LANES
    rows = tile_rows * group
    blocks = depth // rows
    k = lax.axis_index("depth")
    me = lax.axis_index("lat")
    q = lax.rem(me, group)
    base = me - q
    has_up, has_down = base > 0, base + group < lat_count
    has_left, has_right = q > 0, q < group - 1

    above_below[...] = jnp.zeros_like(above_below)
    sides[...] = jnp.zeros_like(sides)

    barrier = pltpu.get_barrier_semaphore()

    def greet(device):
        pl.semaphore_signal(barrier, inc=1, device_id=device, device_id_type=MESH)

    greet((1 - k, me))
    for offset in range(1, group):
        greet((k, base + lax.rem(q + offset, group)))
    pl.when(has_up)(lambda: greet((k, me - group)))
    pl.when(has_down)(lambda: greet((k, me + group)))
    pl.semaphore_wait(barrier, group + has_up.astype(jnp.int32) + has_down.astype(jnp.int32))

    def columns(index):
        return pl.ds(pl.multiple_of(index * LANES, LANES), LANES)

    def remote(src_ref, dst_ref, send, recv, device):
        return pltpu.make_async_remote_copy(
            src_ref=src_ref, dst_ref=dst_ref, send_sem=send, recv_sem=recv, device_id=device, device_id_type=MESH
        )

    def incoming(which, given, landing, offset):
        partner = lax.rem(q + offset, group)
        return remote(
            given.at[:, :, columns(partner)], landing.at[pl.ds(q * tile_rows, tile_rows)],
            in_send.at[which, offset], in_recv.at[which, offset], (k, base + partner),
        )

    pairs = ((temp, field.at[0]), (source, src))
    own = []
    for which, (given, landing) in enumerate(pairs):
        for offset in range(1, group):
            incoming(which, given, landing, offset).start()
        own.append(pltpu.make_async_copy(
            given.at[:, :, columns(q)], landing.at[pl.ds(q * tile_rows, tile_rows)], local_sem.at[which]
        ))
        own[-1].start()

    high, low = halves(inverse[...])
    matrix[:depth, :depth] = high
    matrix[:depth, depth:] = high
    matrix[depth:, :depth] = low
    matrix[depth:, depth:] = jnp.zeros_like(low)
    weights[...] = jnp.transpose(jnp.broadcast_to(couple[...], (LANES, depth)))

    lane = lax.broadcasted_iota(jnp.int32, (rows, LANES), 1)
    first_lane = lax.broadcasted_iota(jnp.int32, (depth, LANES), 1) == 0
    last_lane = lax.broadcasted_iota(jnp.int32, (depth, LANES), 1) == LANES - 1
    edge_layer = jnp.where(k == 0, depth - 1, 0)
    face_gain = jnp.where(lax.broadcasted_iota(jnp.int32, (depth, LANES), 0) == edge_layer, face[0], 0.0)

    def row_copy(slot, parity):
        if slot == 0:
            return remote(field.at[parity, rows - 1], above_below.at[parity, 0], row_send.at[parity, 0],
                          row_recv.at[parity, 0], (k, me + group))
        return remote(field.at[parity, 0], above_below.at[parity, 1], row_send.at[parity, 1],
                      row_recv.at[parity, 1], (k, me - group))

    def side_copy(slot, parity):
        return remote(side_out.at[slot], sides.at[parity, slot], side_send.at[parity, slot],
                      side_recv.at[parity, slot], (k, me + 1 if slot == 0 else me - 1))

    def layer_copy():
        return remote(layer_out, layer, layer_send, layer_recv, (1 - k, me))

    goes = (has_down, has_up)
    comes = (has_up, has_down)
    side_goes = (has_right, has_left)
    side_comes = (has_left, has_right)

    def start_rows(parity):
        for slot in range(2):
            pl.when(goes[slot])(lambda slot=slot: row_copy(slot, parity).start())

    def start_sides(parity):
        for slot in range(2):
            pl.when(side_goes[slot])(lambda slot=slot: side_copy(slot, parity).start())

    def finish_halo(parity):
        for slot in range(2):
            pl.when(comes[slot])(lambda slot=slot: row_copy(slot, parity).wait_recv())
            pl.when(goes[slot])(lambda slot=slot: row_copy(slot, parity).wait_send())
            pl.when(side_comes[slot])(lambda slot=slot: side_copy(slot, parity).wait_recv())
            pl.when(side_goes[slot])(lambda slot=slot: side_copy(slot, parity).wait_send())

    def pack(row, value, packed):
        right, left = packed
        for block in range(blocks):
            place = block * rows + row
            part = value[block * rows:(block + 1) * rows]
            at = lane == place
            right = jnp.where(at, pltpu.roll(part, (place + 1) % LANES, 1), right)
            left = jnp.where(at, pltpu.roll(part, place, 1) if place else part, left)
        return right, left

    def unpack(slot_value, row, lane_at):
        parts = []
        for block in range(blocks):
            shift = (lane_at - block * rows - row) % LANES
            parts.append(pltpu.roll(slot_value, shift, 1) if shift else slot_value)
        return jnp.concatenate(parts, axis=0)

    def keep_layer(row, value):
        layer_out[row:row + 1, :] = jnp.where(k == 0, value[depth - 1:depth], value[0:1])

    nothing = (jnp.zeros((rows, LANES), F32), jnp.zeros((rows, LANES), F32))

    own[0].wait()
    for offset in range(1, group):
        incoming(0, temp, field.at[0], offset).wait()
    start_rows(0)
    packed = nothing
    for row in range(rows):
        value = field[0, row]
        packed = pack(row, value, packed)
        keep_layer(row, value)
    side_out[0], side_out[1] = packed
    start_sides(0)
    pl.when(k == 1)(lambda: layer_copy().start())
    own[1].wait()
    for offset in range(1, group):
        incoming(1, source, src, offset).wait()

    order = [(0, rows - 1)] + [(row, row + 1) for row in range(1, rows - 1, 2)]

    def sweep(step, carry):
        parity = lax.rem(step, 2)
        later = 1 - parity
        finish_halo(parity)
        pl.when((k == 1) | (step > 0))(lambda: layer_copy().wait_send())
        layer_copy().wait_recv()
        other = layer[...]
        from_left, from_right = sides[parity, 0], sides[parity, 1]
        packed = nothing
        for number, pair in enumerate(order):
            sums = []
            for row in pair:
                here = field[parity, row]
                up = field[parity, row - 1] if row > 0 else above_below[parity, 0]
                down = field[parity, row + 1] if row < rows - 1 else above_below[parity, 1]
                before = jnp.where(first_lane, unpack(from_left, row, 0), pltpu.roll(here, 1, 1))
                after = jnp.where(last_lane, unpack(from_right, row, LANES - 1), pltpu.roll(here, LANES - 1, 1))
                right_side = src[row] + weights[...] * ((up + down) + (before + after))
                sums.append(right_side + face_gain * other[row:row + 1])
            high, low = halves(jnp.concatenate(sums, axis=1))
            product = jnp.dot(matrix[...], jnp.concatenate([high, low], axis=0), preferred_element_type=F32)
            solved = product[:depth] + product[depth:]
            for at, row in enumerate(pair):
                value = solved[:, at * LANES:(at + 1) * LANES]
                field[later, row] = value
                packed = pack(row, value, packed)
                keep_layer(row, value)
            if number == 0:
                pl.when(step < SWEEPS - 1)(lambda: start_rows(later))
        pl.when((k == 0) | (step < SWEEPS - 1))(lambda: layer_copy().start())
        side_out[0], side_out[1] = packed
        pl.when(step < SWEEPS - 1)(lambda: start_sides(later))
        return carry

    lax.fori_loop(0, SWEEPS, sweep, 0)

    final = SWEEPS % 2

    def outgoing(offset):
        partner = lax.rem(q + offset, group)
        return remote(
            field.at[final, pl.ds(partner * tile_rows, tile_rows)], out.at[:, :, columns(q)],
            out_send.at[offset], out_recv.at[offset], (k, base + partner),
        )

    for offset in range(1, group):
        outgoing(offset).start()
    mine = pltpu.make_async_copy(
        field.at[final, pl.ds(q * tile_rows, tile_rows)], out.at[:, :, columns(q)], local_sem.at[0]
    )
    mine.start()
    pl.when(k == 0)(lambda: layer_copy().wait_send())
    for offset in range(1, group):
        outgoing(offset).wait()
    mine.wait()


def solution(mesh):
    lat_count = mesh.shape["lat"]

    def local(temp_old, source, lat_couple, face_couple, block_inverse):
        depth, tile_rows, cols = temp_old.shape
        group = cols // LANES
        rows = tile_rows * group
        vmem = pl.BlockSpec(memory_space=pltpu.VMEM)
        dma = pltpu.SemaphoreType.DMA
        result = pl.pallas_call(
            functools.partial(kernel, lat_count),
            out_shape=jax.ShapeDtypeStruct((tile_rows, depth, cols), F32),
            in_specs=[vmem, vmem, vmem, pl.BlockSpec(memory_space=pltpu.SMEM), vmem],
            out_specs=vmem,
            scratch_shapes=[
                pltpu.VMEM((2, rows, depth, LANES), F32),
                pltpu.VMEM((rows, depth, LANES), F32),
                pltpu.VMEM((2, 2, depth, LANES), F32),
                pltpu.VMEM((2, 2, rows, LANES), F32),
                pltpu.VMEM((rows, LANES), F32),
                pltpu.VMEM((2, rows, LANES), F32),
                pltpu.VMEM((rows, LANES), F32),
                pltpu.VMEM((depth, LANES), F32),
                pltpu.VMEM((2 * depth, 2 * depth), BF16),
                dma((2,)),
                dma((2, group)), dma((2, group)),
                dma((2, 2)), dma((2, 2)),
                dma((2, 2)), dma((2, 2)),
                dma, dma,
                dma((group,)), dma((group,)),
            ],
            compiler_params=pltpu.CompilerParams(collective_id=0, has_side_effects=True),
        )(
            jnp.transpose(temp_old, (1, 0, 2)), jnp.transpose(source, (1, 0, 2)),
            lat_couple.reshape(1, depth), face_couple, block_inverse,
        )
        return jnp.transpose(result, (1, 0, 2))

    return jax.shard_map(
        local,
        mesh=mesh,
        in_specs=(P("depth", "lat", None), P("depth", "lat", None), P("depth"), P(), P("depth", None)),
        out_specs=P("depth", "lat", None),
        check_vma=False,
    )
```

```python
import functools

import jax
import jax.numpy as jnp
from jax import lax
from jax.experimental import pallas as pl
from jax.experimental.pallas import tpu as pltpu
from jax.sharding import PartitionSpec as P

SWEEPS = 6
LANES = 128
SUBLANES = 8
MESH = pl.DeviceIdType.MESH
F32, BF16 = jnp.float32, jnp.bfloat16


def halves(value):
    high = value.astype(BF16)
    return high, (value - high.astype(F32)).astype(BF16)


def kernel(lat_count, temp, source, couple, face, inverse, out, field, src, above_below, sides, layer,
           side_out, layer_out, weights, matrix, local_sem, in_send, in_recv, row_send, row_recv,
           side_send, side_recv, layer_send, layer_recv, out_send, out_recv):
    tile_rows, depth, cols = temp.shape
    group = cols // LANES
    rows = tile_rows * group
    order = [(0, rows - 1)] + [(row, row + 1) for row in range(1, rows - 1, 2)]
    turn = [row for pair in order for row in pair]
    layer_rows, side_rows = layer.shape[0], sides.shape[2]
    layer_rows, side_rows = rows // layer_rows, rows // side_rows
    blocks = depth // SUBLANES
    k = lax.axis_index("depth")
    me = lax.axis_index("lat")
    q = lax.rem(me, group)
    base = me - q
    has_up, has_down = base > 0, base + group < lat_count
    has_left, has_right = q > 0, q < group - 1

    above_below[...] = jnp.zeros_like(above_below)
    sides[...] = jnp.zeros_like(sides)

    barrier = pltpu.get_barrier_semaphore()

    def greet(device):
        pl.semaphore_signal(barrier, inc=1, device_id=device, device_id_type=MESH)

    greet((1 - k, me))
    for offset in range(1, group):
        greet((k, base + lax.rem(q + offset, group)))
    pl.when(has_up)(lambda: greet((k, me - group)))
    pl.when(has_down)(lambda: greet((k, me + group)))
    pl.semaphore_wait(barrier, group + has_up.astype(jnp.int32) + has_down.astype(jnp.int32))

    def columns(index):
        return pl.ds(pl.multiple_of(index * LANES, LANES), LANES)

    def remote(src_ref, dst_ref, send, recv, device):
        return pltpu.make_async_remote_copy(
            src_ref=src_ref, dst_ref=dst_ref, send_sem=send, recv_sem=recv, device_id=device, device_id_type=MESH
        )

    def incoming(which, given, landing, offset):
        partner = lax.rem(q + offset, group)
        return remote(
            given.at[:, :, columns(partner)], landing.at[pl.ds(q * tile_rows, tile_rows)],
            in_send.at[which, offset], in_recv.at[which, offset], (k, base + partner),
        )

    pairs = ((temp, field.at[0]), (source, src))
    own = []
    for which, (given, landing) in enumerate(pairs):
        for offset in range(1, group):
            incoming(which, given, landing, offset).start()
        own.append(pltpu.make_async_copy(
            given.at[:, :, columns(q)], landing.at[pl.ds(q * tile_rows, tile_rows)], local_sem.at[which]
        ))
        own[-1].start()

    high, low = halves(inverse[...])
    matrix[:depth, :depth] = high
    matrix[:depth, depth:] = high
    matrix[depth:, :depth] = low
    matrix[depth:, depth:] = jnp.zeros_like(low)
    weights[...] = jnp.transpose(jnp.broadcast_to(couple[...], (LANES, depth)))

    lane = lax.broadcasted_iota(jnp.int32, (SUBLANES, LANES), 1)
    first_lane = lax.broadcasted_iota(jnp.int32, (depth, LANES), 1) == 0
    last_lane = lax.broadcasted_iota(jnp.int32, (depth, LANES), 1) == LANES - 1
    edge_layer = jnp.where(k == 0, depth - 1, 0)
    face_gain = jnp.where(lax.broadcasted_iota(jnp.int32, (depth, LANES), 0) == edge_layer, face[0], 0.0)

    def row_copy(slot, parity):
        if slot == 0:
            return remote(field.at[parity, rows - 1], above_below.at[parity, 0], row_send.at[parity, 0],
                          row_recv.at[parity, 0], (k, me + group))
        return remote(field.at[parity, 0], above_below.at[parity, 1], row_send.at[parity, 1],
                      row_recv.at[parity, 1], (k, me - group))

    def side_copy(slot, parity, chunk):
        return remote(side_out.at[slot, chunk], sides.at[parity, slot, chunk], side_send.at[parity, slot, chunk],
                      side_recv.at[parity, slot, chunk], (k, me + 1 if slot == 0 else me - 1))

    def layer_copy(chunk):
        return remote(layer_out.at[chunk], layer.at[chunk], layer_send.at[chunk], layer_recv.at[chunk], (1 - k, me))

    goes = (has_down, has_up)
    comes = (has_up, has_down)
    side_goes = (has_right, has_left)
    side_comes = (has_left, has_right)

    def start_rows(parity):
        for slot in range(2):
            pl.when(goes[slot])(lambda slot=slot: row_copy(slot, parity).start())

    def start_sides(parity, chunk):
        for slot in range(2):
            pl.when(side_goes[slot])(lambda slot=slot: side_copy(slot, parity, chunk).start())

    def finish_rows(parity):
        for slot in range(2):
            pl.when(comes[slot])(lambda slot=slot: row_copy(slot, parity).wait_recv())
            pl.when(goes[slot])(lambda slot=slot: row_copy(slot, parity).wait_send())

    def finish_sides(parity, chunk):
        for slot in range(2):
            pl.when(side_comes[slot])(lambda slot=slot: side_copy(slot, parity, chunk).wait_recv())
            pl.when(side_goes[slot])(lambda slot=slot: side_copy(slot, parity, chunk).wait_send())

    def pack(index, value, packed):
        right, left = packed
        for block in range(blocks):
            place = block * side_rows + index % side_rows
            part = value[block * SUBLANES:(block + 1) * SUBLANES]
            at = lane == place
            right = jnp.where(at, pltpu.roll(part, (place + 1) % LANES, 1) if place < LANES - 1 else part, right)
            left = jnp.where(at, pltpu.roll(part, place, 1) if place else part, left)
        return right, left

    def unpack(slot_value, index, lane_at):
        parts = []
        for block in range(blocks):
            shift = (lane_at - block * side_rows - index % side_rows) % LANES
            parts.append(pltpu.roll(slot_value, shift, 1) if shift else slot_value)
        return jnp.concatenate(parts, axis=0)

    def keep_layer(index, value):
        at = index % layer_rows
        layer_out[index // layer_rows, at:at + 1, :] = jnp.where(k == 0, value[depth - 1:depth], value[0:1])

    nothing = (jnp.zeros((SUBLANES, LANES), F32), jnp.zeros((SUBLANES, LANES), F32))

    own[0].wait()
    for offset in range(1, group):
        incoming(0, temp, field.at[0], offset).wait()
    start_rows(0)
    for index, row in enumerate(turn):
        value = field[0, row]
        packed = pack(index, value, nothing if index % side_rows == 0 else packed)
        keep_layer(index, value)
        if (index + 1) % layer_rows == 0:
            pl.when(k == 1)(lambda chunk=index // layer_rows: layer_copy(chunk).start())
        if (index + 1) % side_rows == 0:
            chunk = index // side_rows
            side_out[0, chunk], side_out[1, chunk] = packed
            start_sides(0, chunk)
    own[1].wait()
    for offset in range(1, group):
        incoming(1, source, src, offset).wait()

    def sweep(step, carry):
        parity = lax.rem(step, 2)
        later = 1 - parity
        finish_rows(parity)
        for number, pair in enumerate(order):
            first = number * 2
            chunk = first // side_rows
            if first % side_rows == 0:
                finish_sides(parity, chunk)
                packed = nothing
                from_left, from_right = sides[parity, 0, chunk], sides[parity, 1, chunk]
            group_of = first // layer_rows
            if first % layer_rows == 0:
                pl.when((k == 1) | (step > 0))(lambda group_of=group_of: layer_copy(group_of).wait_send())
                layer_copy(group_of).wait_recv()
                other = layer[group_of]
            sums = []
            for index, row in enumerate(pair, first):
                here = field[parity, row]
                up = field[parity, row - 1] if row > 0 else above_below[parity, 0]
                down = field[parity, row + 1] if row < rows - 1 else above_below[parity, 1]
                before = jnp.where(first_lane, unpack(from_left, index, 0), pltpu.roll(here, 1, 1))
                after = jnp.where(last_lane, unpack(from_right, index, LANES - 1), pltpu.roll(here, LANES - 1, 1))
                right_side = src[row] + weights[...] * ((up + down) + (before + after))
                at = index % layer_rows
                sums.append(right_side + face_gain * other[at:at + 1])
            high, low = halves(jnp.concatenate(sums, axis=1))
            product = jnp.dot(matrix[...], jnp.concatenate([high, low], axis=0), preferred_element_type=F32)
            solved = product[:depth] + product[depth:]
            for at, row in enumerate(pair):
                value = solved[:, at * LANES:(at + 1) * LANES]
                field[later, row] = value
                packed = pack(first + at, value, packed)
                keep_layer(first + at, value)
            if number == 0:
                pl.when(step < SWEEPS - 1)(lambda: start_rows(later))
            if (first + 2) % layer_rows == 0:
                pl.when((k == 0) | (step < SWEEPS - 1))(lambda group_of=group_of: layer_copy(group_of).start())
            if (first + 2) % side_rows == 0:
                side_out[0, chunk], side_out[1, chunk] = packed
                pl.when(step < SWEEPS - 1)(lambda chunk=chunk: start_sides(later, chunk))
        return carry

    lax.fori_loop(0, SWEEPS, sweep, 0)

    final = SWEEPS % 2

    def outgoing(offset):
        partner = lax.rem(q + offset, group)
        return remote(
            field.at[final, pl.ds(partner * tile_rows, tile_rows)], out.at[:, :, columns(q)],
            out_send.at[offset], out_recv.at[offset], (k, base + partner),
        )

    for offset in range(1, group):
        outgoing(offset).start()
    mine = pltpu.make_async_copy(
        field.at[final, pl.ds(q * tile_rows, tile_rows)], out.at[:, :, columns(q)], local_sem.at[0]
    )
    mine.start()
    for chunk in range(layer.shape[0]):
        pl.when(k == 0)(lambda chunk=chunk: layer_copy(chunk).wait_send())
    for offset in range(1, group):
        outgoing(offset).wait()
    mine.wait()


def solution(mesh):
    lat_count = mesh.shape["lat"]

    def local(temp_old, source, lat_couple, face_couple, block_inverse):
        depth, tile_rows, cols = temp_old.shape
        group = cols // LANES
        rows = tile_rows * group
        side_chunks = rows * depth // (SUBLANES * LANES)
        layer_chunks = rows // 4
        vmem = pl.BlockSpec(memory_space=pltpu.VMEM)
        dma = pltpu.SemaphoreType.DMA
        result = pl.pallas_call(
            functools.partial(kernel, lat_count),
            out_shape=jax.ShapeDtypeStruct((tile_rows, depth, cols), F32),
            in_specs=[vmem, vmem, vmem, pl.BlockSpec(memory_space=pltpu.SMEM), vmem],
            out_specs=vmem,
            scratch_shapes=[
                pltpu.VMEM((2, rows, depth, LANES), F32),
                pltpu.VMEM((rows, depth, LANES), F32),
                pltpu.VMEM((2, 2, depth, LANES), F32),
                pltpu.VMEM((2, 2, side_chunks, SUBLANES, LANES), F32),
                pltpu.VMEM((layer_chunks, SUBLANES, LANES), F32),
                pltpu.VMEM((2, side_chunks, SUBLANES, LANES), F32),
                pltpu.VMEM((layer_chunks, SUBLANES, LANES), F32),
                pltpu.VMEM((depth, LANES), F32),
                pltpu.VMEM((2 * depth, 2 * depth), BF16),
                dma((2,)),
                dma((2, group)), dma((2, group)),
                dma((2, 2)), dma((2, 2)),
                dma((2, 2, side_chunks)), dma((2, 2, side_chunks)),
                dma((layer_chunks,)), dma((layer_chunks,)),
                dma((group,)), dma((group,)),
            ],
            compiler_params=pltpu.CompilerParams(collective_id=0, has_side_effects=True),
        )(
            jnp.transpose(temp_old, (1, 0, 2)), jnp.transpose(source, (1, 0, 2)),
            lat_couple.reshape(1, depth), face_couple, block_inverse,
        )
        return jnp.transpose(result, (1, 0, 2))

    return jax.shard_map(
        local,
        mesh=mesh,
        in_specs=(P("depth", "lat", None), P("depth", "lat", None), P("depth"), P(), P("depth", None)),
        out_specs=P("depth", "lat", None),
        check_vma=False,
    )
```
